32 devices in a mesh: ctx: 16 (over z, y, core), head: 2 (over x).
Axes of the slice: x: 2, y: 2, z: 4, core: 2. Of those that a mesh axis runs over, the one named last changes fastest.
Arguments:
- hidden: bfloat16 [2048, 8192], P('ctx', 'head'), may hold values from -6 to 6
- query: bfloat16 [2048, 8192], P('ctx', 'head'), may hold values from -60 to 60
- fresh_key_value: bfloat16 [2, 2048, 1024], P(None, 'ctx', 'head'), may hold values from -6 to 6
- cached_key_value: bfloat16 [2, 4096, 1024], P(None, 'ctx', 'head'), may hold values from -6 to 6
- positions: int32 [3, 2048], P(None, 'ctx'), may hold values from 0 to 4095
- out_weight: bfloat16 [8192, 8192], P('head', 'ctx'), may hold values from -0.0625 to 0.0625
- norm_gain: float32 [8192], P('head'), may hold values from 0.25 to 1.75
- layer3_key_value_weight: bfloat16 [8192, 2048], P(None, 'head'), may hold values from -0.0625 to 0.0625
- layer3_key_value_bias: float32 [2048], P('head'), may hold values from -3 to 3
- keep_index: int32 [2048], P('ctx'), may hold values from 0 to 127, as said below
- keep_count: int32 [16], P('ctx'), may hold values from 64 to 128, as said below
Outputs:
- layer2_out: bfloat16 [2048, 8192], P('ctx', 'head')
- layer3_packed_key_value: bfloat16 [2048, 2048], P('ctx', 'head')
The draws below stay inside these ranges and needn't reach their ends.
Inputs may be any that keep to these rules, and one draw needn't show every extreme that they name: `keep_index`: within each block of 128 entries, the first keep_count entries are the kept rows in rising order (all text rows and every second visual row), the rest the dropped rows in rising order. `keep_count`: some block keeps all 128 rows in every draw.
All inputs are finite; a program needn't handle non-finite values.
Results may differ from the reference program's by a relative error of at most 0.012.
Values may be sent and summed in bfloat16 or wider, within the bound.
A program may use at most 192 MiB of HBM per device.

```python
import jax
import jax.numpy as jnp
from jax import lax

MODEL_WIDTH = 8192
QUERY_HEADS = 64
KEY_VALUE_HEADS = 8
HEAD_DIMENSION = 128
FRESH_TOKENS = 128
FRESH_TOTAL = 2048
CACHED_TOKENS = 4096


def keep_tables(key):
    block_list = FRESH_TOTAL // FRESH_TOKENS
    first_key, second_key, third_key = jax.random.split(jax.random.fold_in(key, 71), 3)
    visual_share = jax.random.randint(first_key, (block_list, 1), 0, FRESH_TOKENS + 1)
    visual = jax.random.randint(second_key, (block_list, FRESH_TOKENS), 0, FRESH_TOKENS) < visual_share
    chosen_block = jax.random.randint(third_key, (), 0, block_list)
    visual = visual & (jnp.arange(block_list)[:, None] != chosen_block)
    visual_rank = jnp.cumsum(visual.astype(jnp.int32), axis=1) - 1
    dropped = visual & (visual_rank % 2 == 1)
    sort_keys = dropped.astype(jnp.int32) * FRESH_TOKENS + jnp.arange(FRESH_TOKENS, dtype=jnp.int32)[None, :]
    kept_order = jnp.argsort(sort_keys, axis=1, stable=True).astype(jnp.int32)
    kept_count = (FRESH_TOKENS - jnp.sum(dropped.astype(jnp.int32), axis=1)).astype(jnp.int32)
    return (kept_order.reshape(-1), kept_count)


def draw_keep_index(key, part):
    return keep_tables(key)[0]


def draw_keep_count(key, part):
    return keep_tables(key)[1]


def draw_query(key, part):
    first_key = jax.random.fold_in(jax.random.fold_in(key, 13), 0)
    shape = (FRESH_TOTAL, QUERY_HEADS * HEAD_DIMENSION)
    values = jax.random.normal(first_key, shape, jnp.float32)
    return jnp.clip(values, -60.0, 60.0).astype(jnp.bfloat16)


def set_ends(result, key, least, top_value):
    extent = result.shape
    spot = [jax.random.randint(jax.random.fold_in(key, axis), (), 0, extent[axis]) for axis in range(len(extent))]
    result = result.at[tuple(spot)].set(least)
    longest = extent.index(max(extent))
    spot[longest] = (spot[longest] + 1) % extent[longest]
    return result.at[tuple(spot)].set(top_value)


def block_scale(key, shape, pieces, low, high):
    level, own = 1.0, jax.random.fold_in(key, 6)
    for dim, shards_of in pieces:
        steps = jnp.exp(jax.random.uniform(jax.random.fold_in(own, dim), (shards_of,), jnp.float32, low / len(pieces), high / len(pieces)))
        level = level * jnp.repeat(steps, shape[dim] // shards_of).reshape([-1 if axis == dim else 1 for axis in range(len(shape))])
    return level


def normal_values(key, extent, deviation, bound, cuts=(), kind=jnp.bfloat16):
    values = deviation * jax.random.normal(key, extent, jnp.float32)
    if cuts:
        values = values * block_scale(key, extent, cuts, -0.22, 0.18)
    return jnp.clip(values, -bound, bound).astype(kind)


def setup_inputs(seed: int = 0) -> dict:
    streams_of = jax.random.split(jax.random.key(seed), 12)
    return {
        "hidden": normal_values(streams_of[0], (FRESH_TOTAL, MODEL_WIDTH), 1.0, 6.0, ((0, 16), (1, 2))),
        "query": draw_query(jax.random.fold_in(streams_of[11], 71), 0),
        "fresh_key_value": normal_values(streams_of[2], (2, FRESH_TOTAL, KEY_VALUE_HEADS * HEAD_DIMENSION), 1.0, 6.0, ((1, 16), (2, 2))),
        "cached_key_value": normal_values(streams_of[3], (2, CACHED_TOKENS, KEY_VALUE_HEADS * HEAD_DIMENSION), 1.0, 6.0, ((1, 16), (2, 2))),
        "positions": set_ends(jax.random.randint(streams_of[4], (3, FRESH_TOTAL), 0, 4096), jax.random.fold_in(streams_of[4], 1), 0, 4095).astype(jnp.int32),
        "out_weight": normal_values(streams_of[5], (QUERY_HEADS * HEAD_DIMENSION, MODEL_WIDTH), (QUERY_HEADS * HEAD_DIMENSION) ** -0.5, 0.0625, ((0, 2), (1, 16))),
        "norm_gain": jnp.clip(1.0 + 0.15 * jax.random.normal(streams_of[6], (MODEL_WIDTH,), jnp.float32), 0.25, 1.75),
        "layer3_key_value_weight": normal_values(streams_of[7], (MODEL_WIDTH, 2 * KEY_VALUE_HEADS * HEAD_DIMENSION), MODEL_WIDTH ** -0.5, 0.0625, ((1, 2),)),
        "layer3_key_value_bias": normal_values(streams_of[8], (2 * KEY_VALUE_HEADS * HEAD_DIMENSION,), 0.5, 3.0, ((0, 2),), jnp.float32),
        "keep_index": draw_keep_index(jax.random.fold_in(streams_of[11], 71), 0),
        "keep_count": draw_keep_count(jax.random.fold_in(streams_of[11], 71), 0),
    }


def tables(positions, head_size):
    half = head_size // 2
    column = jnp.arange(half)
    frequency = jnp.power(jnp.float32(1000000.0), -(2.0 * column.astype(jnp.float32)) / head_size)
    section = (column >= head_size // 8).astype(jnp.int32) + (column >= head_size // 8 + 3 * head_size // 16).astype(jnp.int32)
    places = positions.astype(jnp.float32)
    chosen = jnp.where(section[None, :] == 0, places[0][:, None], jnp.where(section[None, :] == 1, places[1][:, None], places[2][:, None]))
    angles = chosen * frequency[None, :]
    return (jnp.cos(angles), jnp.sin(angles))

def apply_rotary(x, cosine_table, sine_table):
    half = x.shape[-1] // 2
    first_half = x[..., :half]
    second_half = x[..., half:]
    cosine_table = cosine_table[:, None, :]
    sine_table = sine_table[:, None, :]
    return jnp.concatenate([first_half * cosine_table - second_half * sine_table, second_half * cosine_table + first_half * sine_table], axis=-1)

def reference(hidden, query, fresh_key_value, cached_key_value, positions, out_weight, norm_gain, layer3_key_value_weight, layer3_key_value_bias, keep_index, keep_count):
    fresh_token_count = hidden.shape[0]
    block_list = fresh_token_count // FRESH_TOKENS
    query_group_width = QUERY_HEADS // KEY_VALUE_HEADS
    cosine_table, sine_table = tables(positions, HEAD_DIMENSION)
    rotary_query_rows = apply_rotary(query.astype(jnp.float32).reshape(fresh_token_count, QUERY_HEADS, HEAD_DIMENSION), cosine_table, sine_table).astype(jnp.bfloat16)
    rotary_key_rows = apply_rotary(fresh_key_value[0].astype(jnp.float32).reshape(fresh_token_count, KEY_VALUE_HEADS, HEAD_DIMENSION), cosine_table, sine_table).astype(jnp.bfloat16)
    key_matrix_rows = jnp.concatenate([cached_key_value[0].reshape(CACHED_TOKENS, KEY_VALUE_HEADS, HEAD_DIMENSION), rotary_key_rows], axis=0).transpose(1, 0, 2)
    value_matrix_rows = jnp.concatenate([cached_key_value[1].reshape(CACHED_TOKENS, KEY_VALUE_HEADS, HEAD_DIMENSION), fresh_key_value[1].reshape(fresh_token_count, KEY_VALUE_HEADS, HEAD_DIMENSION)], axis=0).transpose(1, 0, 2)
    grouped_rows = rotary_query_rows.reshape(block_list, FRESH_TOKENS, KEY_VALUE_HEADS, query_group_width, HEAD_DIMENSION).transpose(0, 2, 1, 3, 4)

    def per_block(inputs):
        query_block, block_number = inputs
        query_pos = block_number * FRESH_TOKENS + jnp.arange(FRESH_TOKENS)
        recent = jnp.arange(fresh_token_count)[None, :] <= query_pos[:, None]
        visible = jnp.concatenate([jnp.ones((FRESH_TOKENS, CACHED_TOKENS), bool), recent], axis=1)

        def per_head(head_inputs):
            query_head, key_head, value_head = head_inputs
            scores = jnp.einsum('ngd,ld->ngl', query_head.astype(jnp.float32), key_head.astype(jnp.float32)) * HEAD_DIMENSION ** (-0.5)
            scores = jnp.where(visible[:, None, :], scores, -jnp.inf)
            maxima = lax.optimization_barrier(jnp.max(scores, axis=-1, keepdims=True))
            expos = jnp.exp(scores - maxima)
            totals = lax.optimization_barrier(jnp.sum(expos, axis=-1))
            weights = expos.astype(jnp.bfloat16)
            summed = jnp.einsum('ngl,ld->ngd', weights.astype(jnp.float32), value_head.astype(jnp.float32))
            return summed / totals[..., None]
        return lax.map(per_head, (query_block, key_matrix_rows, value_matrix_rows))
    outputs = lax.map(per_block, (grouped_rows, jnp.arange(block_list)))
    attn = outputs.transpose(0, 2, 1, 3, 4).reshape(fresh_token_count, QUERY_HEADS * HEAD_DIMENSION).astype(jnp.bfloat16)
    projection = jnp.dot(attn, out_weight, preferred_element_type=jnp.float32)
    layer2_out = (hidden.astype(jnp.float32) + projection).astype(jnp.bfloat16)
    widened = layer2_out.astype(jnp.float32)
    mean_square = lax.optimization_barrier(jnp.mean(widened * widened, axis=1))
    normalized_rows = (widened * lax.rsqrt(mean_square + 1e-06)[:, None] * norm_gain).astype(jnp.bfloat16)
    layer_three_key_value = (jnp.dot(normalized_rows, layer3_key_value_weight, preferred_element_type=jnp.float32) + layer3_key_value_bias).reshape(fresh_token_count, KEY_VALUE_HEADS, 2, HEAD_DIMENSION)
    layer_three_keys = apply_rotary(layer_three_key_value[:, :, 0], cosine_table, sine_table)
    layer_three_key_value = jnp.stack([layer_three_keys, layer_three_key_value[:, :, 1]], axis=2).reshape(fresh_token_count, 2 * KEY_VALUE_HEADS * HEAD_DIMENSION).astype(jnp.bfloat16)
    grouped_by_block = layer_three_key_value.reshape(block_list, FRESH_TOKENS, 2 * KEY_VALUE_HEADS * HEAD_DIMENSION)
    indices = keep_index.reshape(block_list, FRESH_TOKENS).astype(jnp.int32)
    selected_rows = jnp.take_along_axis(grouped_by_block, indices[:, :, None], axis=1)
    block_occupied = jnp.arange(FRESH_TOKENS)[None, :] < keep_count[:, None]
    layer3_packed_key_value = jnp.where(block_occupied[:, :, None], selected_rows, jnp.zeros_like(selected_rows)).reshape(fresh_token_count, 2 * KEY_VALUE_HEADS * HEAD_DIMENSION)
    return (layer2_out, layer3_packed_key_value)
```

```python
import functools

import jax
import jax.numpy as jnp
from jax import lax
from jax.experimental import pallas as pl
from jax.experimental.pallas import tpu as pltpu
from jax.sharding import PartitionSpec as P

HEAD_DIMENSION = 128


def tables(positions, head_size):
    half = head_size // 2
    column = jnp.arange(half)
    frequency = jnp.power(jnp.float32(1000000.0), -(2.0 * column.astype(jnp.float32)) / head_size)
    section = (column >= head_size // 8).astype(jnp.int32) + (
        column >= head_size // 8 + 3 * head_size // 16
    ).astype(jnp.int32)
    places = positions.astype(jnp.float32)
    chosen = jnp.where(
        section[None, :] == 0,
        places[0][:, None],
        jnp.where(section[None, :] == 1, places[1][:, None], places[2][:, None]),
    )
    angles = chosen * frequency[None, :]
    return (jnp.cos(angles), jnp.sin(angles))


def apply_rotary(x, cosine_table, sine_table):
    half = x.shape[-1] // 2
    first_half = x[..., :half]
    second_half = x[..., half:]
    cosine_table = cosine_table[:, None, :]
    sine_table = sine_table[:, None, :]
    return jnp.concatenate(
        [
            first_half * cosine_table - second_half * sine_table,
            second_half * cosine_table + first_half * sine_table,
        ],
        axis=-1,
    )


LOG2E = 1.4426950408889634


def attend_kernel(group, causal, last, row_ref, q_ref, k_ref, v_ref, *rest):
    if last:
        m_in, l_in, a_in, out_ref, m_ref, l_ref, a_ref = rest
    else:
        m_out, l_out, a_out, m_ref, l_ref, a_ref = rest
    step = pl.program_id(1)
    head = k_ref.shape[1]
    rows = q_ref.shape[0]
    block = k_ref.shape[0]

    @pl.when(step == 0)
    def _():
        if last:
            m_ref[...] = m_in[0]
            l_ref[...] = l_in[0]
            a_ref[...] = a_in[0]
        else:
            m_ref[...] = jnp.full_like(m_ref, -1e30)
            l_ref[...] = jnp.zeros_like(l_ref)
            a_ref[...] = jnp.zeros_like(a_ref)

    def update(masked):
        key = k_ref[...]
        value = v_ref[...]
        scale = LOG2E * head ** (-0.5)
        if masked:
            key_pos = step * block + lax.broadcasted_iota(jnp.int32, (rows, block), 1)
            query_pos = row_ref[0] + lax.broadcasted_iota(jnp.int32, (rows, block), 0)
            visible = key_pos <= query_pos
        for g in range(group):
            part = pl.ds(g * rows, rows)
            s = lax.dot_general(
                q_ref[:, g * head : (g + 1) * head],
                key,
                (((1,), (1,)), ((), ())),
                preferred_element_type=jnp.float32,
            )
            if masked:
                s = jnp.where(visible, s, -1e30)
            old = m_ref[part, :]
            new = jnp.maximum(old, jnp.max(s, axis=1, keepdims=True))
            m_ref[part, :] = new
            e = jnp.exp2((s - new[:, :1]) * scale)
            factor = jnp.exp2((old - new) * scale)
            l_ref[part, :] = l_ref[part, :] * factor + jnp.sum(e, axis=1, keepdims=True)
            a_ref[part, :] = a_ref[part, :] * factor + jnp.dot(
                e.astype(jnp.bfloat16), value, preferred_element_type=jnp.float32
            )

    if causal:
        start = step * block

        @pl.when(start + block - 1 <= row_ref[0])
        def _():
            update(False)

        @pl.when((start + block - 1 > row_ref[0]) & (start <= row_ref[0] + rows - 1))
        def _():
            update(True)
    else:
        update(False)

    @pl.when(step == pl.num_programs(1) - 1)
    def _():
        if last:
            for g in range(group):
                part = pl.ds(g * rows, rows)
                out_ref[:, g * head : (g + 1) * head] = (
                    a_ref[part, :] / l_ref[part, :]
                ).astype(out_ref.dtype)
        else:
            m_out[0] = m_ref[...]
            l_out[0] = l_ref[...]
            a_out[0] = a_ref[...]


def attend(query, key_value, first_row, state, head_size):
    rows, width = query.shape
    length = key_value.shape[1]
    kv_local = key_value.shape[2] // head_size
    group = width // head_size // kv_local
    block = 1024
    while length % block:
        block //= 2
    last = state is not None
    high = group * rows
    carry = pl.BlockSpec((1, high, head_size), lambda k, i, r: (k, 0, 0))
    carry_shape = jax.ShapeDtypeStruct((kv_local, high, head_size), jnp.float32)
    wide = pl.BlockSpec((rows, group * head_size), lambda k, i, r: (0, k))
    in_specs = [
        wide,
        pl.BlockSpec((None, block, head_size), lambda k, i, r: (0, i, k)),
        pl.BlockSpec((None, block, head_size), lambda k, i, r: (1, i, k)),
    ] + ([carry] * 3 if last else [])
    operands = (query, key_value, key_value) + (state if last else ())
    return pl.pallas_call(
        functools.partial(attend_kernel, group, last, last),
        out_shape=jax.ShapeDtypeStruct((rows, width), jnp.bfloat16) if last else (carry_shape,) * 3,
        grid_spec=pltpu.PrefetchScalarGridSpec(
            num_scalar_prefetch=1,
            grid=(kv_local, length // block),
            in_specs=in_specs,
            out_specs=wide if last else (carry,) * 3,
            scratch_shapes=[pltpu.VMEM((high, head_size), jnp.float32)] * 3,
        ),
        compiler_params=pltpu.CompilerParams(vmem_limit_bytes=40 * 1024 * 1024),
        cost_estimate=pl.CostEstimate(
            flops=8 * rows * width * length,
            bytes_accessed=4 * length * kv_local * head_size + 4 * rows * width,
            transcendentals=rows * (width // head_size) * length,
        ),
    )(first_row.reshape(1), *operands)


def scatter_kernel(chips, cores, heads, x_ref, o_ref, send_sem, recv_sem, tile, local_sem):
    me = lax.axis_index("ctx")
    h = lax.axis_index("head")
    chip = me // cores
    core = me % cores
    per = chips // heads
    owner_head = chip // per
    slot = h * per + chip % per
    barrier = pltpu.get_barrier_semaphore()
    for d in range(chips):
        there = lax.rem(chip + d, chips) * cores + core
        for e in range(heads):
            if d or e:
                pl.semaphore_signal(
                    barrier,
                    inc=1,
                    device_id=(there, lax.rem(h + e, heads)),
                    device_id_type=pl.DeviceIdType.MESH,
                )
    pl.semaphore_wait(barrier, chips * heads - 1)

    def copy_to(d):
        p = lax.rem(chip + d, chips)
        return pltpu.make_async_remote_copy(
            src_ref=x_ref.at[p],
            dst_ref=o_ref.at[slot],
            send_sem=send_sem.at[d],
            recv_sem=recv_sem.at[slot],
            device_id=(p * cores + core, owner_head),
            device_id_type=pl.DeviceIdType.MESH,
        )

    def receive(s):
        return pltpu.make_async_remote_copy(
            src_ref=x_ref.at[0],
            dst_ref=o_ref.at[s],
            send_sem=send_sem.at[0],
            recv_sem=recv_sem.at[s],
            device_id=(me, lax.rem(h + 1, heads)),
            device_id_type=pl.DeviceIdType.MESH,
        )

    for d in range(1, chips):
        copy_to(d).start()

    @pl.when(owner_head != h)
    def _():
        copy_to(0).start()

    @pl.when(owner_head == h)
    def _():
        into = pltpu.make_async_copy(x_ref.at[chip], tile, local_sem.at[0])
        into.start()
        into.wait()
        out = pltpu.make_async_copy(tile, o_ref.at[slot], local_sem.at[1])
        out.start()
        out.wait()

    for d in range(1, chips):
        copy_to(d).wait_send()

    @pl.when(owner_head != h)
    def _():
        copy_to(0).wait_send()

    for s in range(chips):

        @pl.when(jnp.logical_or(owner_head != h, slot != s))
        def _():
            receive(s).wait_recv()


def scatter_columns(product, chips, cores, heads):
    block = product.shape[1:]
    moved = pl.pallas_call(
        functools.partial(scatter_kernel, chips, cores, heads),
        out_shape=jax.ShapeDtypeStruct(product.shape, product.dtype),
        in_specs=[pl.BlockSpec(memory_space=pl.ANY)],
        out_specs=pl.BlockSpec(memory_space=pl.ANY),
        scratch_shapes=[
            pltpu.SemaphoreType.DMA((chips,)),
            pltpu.SemaphoreType.DMA((chips,)),
            pltpu.VMEM(block, product.dtype),
            pltpu.SemaphoreType.DMA((2,)),
        ],
        compiler_params=pltpu.CompilerParams(collective_id=0, has_side_effects=True),
    )(product)
    return moved.reshape((heads, chips // heads) + block)


def gather_kernel(depth, cores, x_ref, o_ref, send_sem, recv_sem, tile, local_sem):
    me = lax.axis_index("ctx")
    h = lax.axis_index("head")
    chip = me // cores
    core = me % cores
    ring = chip // 2
    side = chip % 2
    pair = ring * 2 + (1 - side)

    def along(d):
        return lax.rem(ring + d, depth)

    barrier = pltpu.get_barrier_semaphore()
    for d in range(1, depth):
        pl.semaphore_signal(
            barrier,
            inc=1,
            device_id=((along(d) * 2 + side) * cores + core, h),
            device_id_type=pl.DeviceIdType.MESH,
        )
    pl.semaphore_signal(
        barrier, inc=1, device_id=(pair * cores + core, h), device_id_type=pl.DeviceIdType.MESH
    )
    pl.semaphore_wait(barrier, depth)

    def send(source, half, origin, target, kind, d):
        return pltpu.make_async_remote_copy(
            src_ref=source,
            dst_ref=o_ref.at[origin, half],
            send_sem=send_sem.at[kind, d],
            recv_sem=recv_sem.at[half, origin],
            device_id=(target * cores + core, h),
            device_id_type=pl.DeviceIdType.MESH,
        )

    def receive(half, origin):
        send(x_ref.at[half], half, origin, pair, 0, 0).wait_recv()

    sent = [send(x_ref.at[0], 0, chip, pair, 0, 0), send(x_ref.at[1], 1, chip, pair, 1, 0)]
    order = [d for pair_of in zip(range(1, depth), range(depth - 1, 0, -1)) for d in pair_of]
    order = list(dict.fromkeys(order))
    for d in order:
        sent.append(send(x_ref.at[1], 1, chip, along(d) * 2 + side, 2, d))
    for d in order:
        sent.append(send(x_ref.at[0], 0, chip, along(d) * 2 + side, 3, d))
    for copy in sent:
        copy.start()
    into = pltpu.make_async_copy(x_ref, tile, local_sem.at[0])
    into.start()
    into.wait()
    out = pltpu.make_async_copy(tile, o_ref.at[chip], local_sem.at[1])
    out.start()

    receive(0, pair)
    for d in order:
        copy = send(o_ref.at[pair, 0], 0, pair, along(d) * 2 + side, 4, d)
        copy.start()
        sent.append(copy)
    for d in order:
        origin = along(d) * 2 + side
        receive(1, origin)
        copy = send(o_ref.at[origin, 1], 1, origin, pair, 1, d)
        copy.start()
        sent.append(copy)
    for d in range(1, depth):
        receive(0, along(d) * 2 + side)
    receive(1, pair)
    for d in range(1, depth):
        receive(0, along(d) * 2 + 1 - side)
        receive(1, along(d) * 2 + 1 - side)
    for copy in sent:
        copy.wait_send()
    out.wait()


def gather_rows(x, chips, cores):
    rows, width = x.shape
    halves = x.reshape(2, rows // 2, width)
    return pl.pallas_call(
        functools.partial(gather_kernel, chips // 2, cores),
        out_shape=jax.ShapeDtypeStruct((chips,) + halves.shape, x.dtype),
        in_specs=[pl.BlockSpec(memory_space=pl.ANY)],
        out_specs=pl.BlockSpec(memory_space=pl.ANY),
        scratch_shapes=[
            pltpu.SemaphoreType.DMA((5, chips // 2)),
            pltpu.SemaphoreType.DMA((2, chips)),
            pltpu.VMEM(halves.shape, x.dtype),
            pltpu.SemaphoreType.DMA((2,)),
        ],
        compiler_params=pltpu.CompilerParams(collective_id=1, has_side_effects=True),
    )(halves).reshape(chips * rows, width)


def exchange(x, axis_name, size):
    return lax.ppermute(x, axis_name, [(i, i ^ 1) for i in range(size)])


def local(
    contexts,
    heads,
    hidden,
    query,
    fresh_key_value,
    cached_key_value,
    positions,
    out_weight,
    norm_gain,
    layer3_key_value_weight,
    layer3_key_value_bias,
    keep_index,
    keep_count,
):
    new_rows = hidden.shape[0]
    head_size = HEAD_DIMENSION
    kv_local = fresh_key_value.shape[2] // head_size
    q_local = query.shape[1] // head_size
    cores = 2
    chips = contexts // cores
    me = lax.axis_index("ctx")
    core = me % cores
    head = lax.axis_index("head")
    cosine_table, sine_table = tables(positions, head_size)
    rotary_query_rows = apply_rotary(
        query.astype(jnp.float32).reshape(new_rows, q_local, head_size), cosine_table, sine_table
    ).astype(jnp.bfloat16).reshape(new_rows, q_local * head_size)
    rotary_key_rows = apply_rotary(
        fresh_key_value[0].astype(jnp.float32).reshape(new_rows, kv_local, head_size),
        cosine_table,
        sine_table,
    ).astype(jnp.bfloat16)
    recent = jnp.stack(
        [rotary_key_rows.reshape(new_rows, kv_local * head_size), fresh_key_value[1]]
    )
    if heads == 2:
        other_gain = exchange(norm_gain, "head", heads)
        whole_gain = jnp.concatenate(
            [jnp.where(head == 0, norm_gain, other_gain), jnp.where(head == 0, other_gain, norm_gain)]
        )
    else:
        whole_gain = lax.all_gather(norm_gain, "head", axis=0, tiled=True)
    other_weight = exchange(out_weight, "ctx", contexts)
    first_row = me * new_rows
    cached_all = lax.all_gather(cached_key_value, "ctx", axis=1, tiled=True)
    recent_all = lax.all_gather(recent, "ctx", axis=1, tiled=True)
    state = attend(rotary_query_rows, cached_all, first_row, None, head_size)
    attn = attend(rotary_query_rows, recent_all, first_row, tuple(state), head_size)
    outputs = gather_rows(attn, chips, cores)
    own = jnp.dot(outputs, out_weight, preferred_element_type=jnp.float32).astype(jnp.bfloat16)
    other = jnp.dot(outputs, other_weight, preferred_element_type=jnp.float32).astype(jnp.bfloat16)
    product = jnp.concatenate(
        [jnp.where(core == 0, own, other), jnp.where(core == 0, other, own)], axis=1
    ).reshape(chips, new_rows, -1)
    parts = scatter_columns(product, chips, cores, heads)
    head_summed = jnp.sum(parts.astype(jnp.float32), axis=0)
    head_summed = head_summed.transpose(1, 0, 2).reshape(hidden.shape)
    layer2_out = (hidden.astype(jnp.float32) + head_summed).astype(jnp.bfloat16)
    if heads == 2:
        other_out = exchange(layer2_out, "head", heads)
        whole_out = jnp.concatenate(
            [
                jnp.where(head == 0, layer2_out, other_out),
                jnp.where(head == 0, other_out, layer2_out),
            ],
            axis=1,
        )
    else:
        whole_out = lax.all_gather(layer2_out, "head", axis=1, tiled=True)
    widened = whole_out.astype(jnp.float32)
    squares = jnp.sum(widened * widened, axis=1)
    level = lax.rsqrt(squares / widened.shape[1] + 1e-06)[:, None]
    full_rows = (widened * level * whole_gain).astype(jnp.bfloat16)
    full_rows = lax.optimization_barrier(full_rows)
    layer_three_key_value = (
        jnp.dot(full_rows, layer3_key_value_weight, preferred_element_type=jnp.float32)
        + layer3_key_value_bias
    ).reshape(new_rows, kv_local, 2, head_size)
    layer_three_keys = apply_rotary(layer_three_key_value[:, :, 0], cosine_table, sine_table)
    layer_three_key_value = (
        jnp.stack([layer_three_keys, layer_three_key_value[:, :, 1]], axis=2)
        .reshape(new_rows, 2 * kv_local * head_size)
        .astype(jnp.bfloat16)
    )
    selected_rows = jnp.take(layer_three_key_value, keep_index, axis=0)
    block_occupied = jnp.arange(new_rows) < keep_count[0]
    layer3_packed_key_value = jnp.where(
        block_occupied[:, None], selected_rows, jnp.zeros_like(selected_rows)
    )
    return (layer2_out, layer3_packed_key_value)


def solution(mesh):
    placed = (
        P("ctx", "head"),
        P("ctx", "head"),
        P(None, "ctx", "head"),
        P(None, "ctx", "head"),
        P(None, "ctx"),
        P("head", "ctx"),
        P("head"),
        P(None, "head"),
        P("head"),
        P("ctx"),
        P("ctx"),
    )
    return jax.shard_map(
        functools.partial(local, mesh.shape["ctx"], mesh.shape["head"]),
        mesh=mesh,
        in_specs=placed,
        out_specs=(P("ctx", "head"), P("ctx", "head")),
        check_vma=False,
    )
```
